256 devices in a mesh: row: 32 (over y, z), col: 8 (over x, core).
Axes of the slice: x: 4, y: 4, z: 8, core: 2. Of those that a mesh axis runs over, the one named last changes fastest.
Arguments:
- grams: bfloat16 [4, 3584, 3584], P(None, 'row', 'col'), as said below
- weights: bfloat16 [4, 3584, 7168], P(None, 'row', 'col'), may hold values from -6 to 6
Outputs:
- merged: float32 [3584, 7168], P('row', 'col')
- residual: float32 [3584, 7168], P('row', 'col')
The draws below stay inside these ranges and needn't reach their ends.
Inputs may be any that keep to these rules, and one draw needn't show every extreme that they name: `grams`: each of the 4 matrices is symmetric and positive definite.
All inputs are finite; a program needn't handle non-finite values.
Results may differ from the reference program's by a relative error of at most 0.012.
The reference program's roundings to bfloat16 on the way (of `rounded`) count: a program that leaves them out, or rounds other values in their place, can miss the bound.
Values may be sent and summed in bfloat16 or wider, within the bound.
No kernel may reach another device: no remote copies, remote signals or barrier semaphores. Data moves between devices by JAX's collectives and lax.ppermute only.
A program may use at most 256 MiB of HBM per device.

```python
import math
import jax
import jax.numpy as jnp
from jax import lax

D = 3584
FF_COLS = 7168
MODELS = 4
ITERS = 2


def draw_grams(key, part):

    def one_model(model_key):
        scale_key, noise_key = jax.random.split(model_key)
        lowest, highest, spread = (0.5, 5.0, 0.3)
        scales = jnp.exp(jax.random.uniform(scale_key, (D,), jnp.float32, math.log(lowest), math.log(highest)))
        roots = jnp.sqrt(scales)
        noise = jax.random.normal(noise_key, (D, D), jnp.float32) * (spread / math.sqrt(D))
        core = jnp.eye(D, dtype=jnp.float32) + (noise + noise.T) * 0.5
        return (core * (roots[:, None] * roots[None, :])).astype(jnp.bfloat16)
    model_keys = jax.random.split(jax.random.fold_in(key, 17), MODELS)
    return jax.vmap(one_model)(model_keys)


def shard_levels(stream_key, shape, cuts, smallest, high):
    def one(position, parts):
        draws = jax.random.uniform(jax.random.fold_in(jax.random.fold_in(stream_key, 6), position), (parts,), jnp.float32, smallest / len(cuts), high / len(cuts))
        return jnp.repeat(jnp.exp(draws), shape[position] // parts).reshape((-1,) + (1,) * (len(shape) - position - 1))

    factor_of = one(*cuts[0])
    for cut in cuts[1:]:
        factor_of = factor_of * one(*cut)
    return factor_of


def bell_draw(rng, shape, width, limit, pieces=(), kind=jnp.bfloat16):
    factor_of = shard_levels(rng, shape, pieces, -0.22, 0.18) if pieces else 1.0
    values = jax.random.normal(rng, shape, jnp.float32) * width * factor_of
    return jnp.minimum(jnp.maximum(values, -limit), limit).astype(kind)


def setup_inputs(seed: int = 0) -> dict:
    streams_of = jax.random.split(jax.random.key(seed), 3)
    return {
        "grams": draw_grams(jax.random.fold_in(streams_of[2], 71), 0),
        "weights": bell_draw(streams_of[1], (MODELS, D, FF_COLS), 1.0, 6.0, ((1, 32), (2, 8))),
    }


def reference(grams, weights):
    high = lax.Precision.HIGHEST
    total = jnp.zeros((D, D), jnp.float32)
    right_side = jnp.zeros((D, FF_COLS), jnp.float32)
    for model_index in range(MODELS):
        gram_full = grams[model_index].astype(jnp.float32)
        weight = weights[model_index].astype(jnp.float32)
        gram_diag = jnp.diagonal(gram_full)
        right_side = right_side + 0.9 * jnp.dot(gram_full, weight, precision=high) + 0.1 * gram_diag[:, None] * weight
        total = total + gram_full
    total_diag = jnp.diagonal(total)
    merged = jnp.zeros((D, FF_COLS), jnp.float32)
    residual = right_side
    direction = right_side
    norm_now = jnp.sum(residual * residual, axis=0)
    for iteration in range(ITERS):
        rounded = lax.optimization_barrier(direction.astype(jnp.bfloat16)).astype(jnp.float32)
        mapped = 0.9 * jnp.dot(total, rounded, precision=high) + 0.1 * total_diag[:, None] * rounded
        curvature = jnp.sum(direction * mapped, axis=0)
        step_length = norm_now / curvature
        merged = merged + step_length * direction
        residual = residual - step_length * mapped
        if iteration + 1 < ITERS:
            norm_next = jnp.sum(residual * residual, axis=0)
            direction = residual + (norm_next / norm_now) * direction
            norm_now = norm_next
    return merged, residual
```

```python
import jax
import jax.numpy as jnp
from jax import lax
from jax.sharding import Mesh
from jax.sharding import PartitionSpec as P


F32, BF16 = jnp.float32, jnp.bfloat16


def shift(x, axis, by):
    size = lax.axis_size(axis)
    return lax.ppermute(x, axis, [(i, (i + by) % size) for i in range(size)])


def all_shifts(x, axis):
    return [x] + [shift(x, axis, by) for by in range(1, lax.axis_size(axis))]


def core_pair(x, axis):
    other = shift(x, "core", 1)
    first = lax.axis_index("core") == 0
    return jnp.concatenate(
        [jnp.where(first, x, other), jnp.where(first, other, x)], axis=axis
    )


def rolled(blocks, start):
    n = blocks.shape[0]
    return [
        lax.dynamic_index_in_dim(blocks, (start + i) % n, 0, keepdims=False) for i in range(n)
    ]


def y_sum(parts):
    return sum(all_shifts(parts, "y"))


def shards(grams, weights):
    y, z, x = (lax.axis_index(a) for a in ("y", "z", "x"))
    core = lax.axis_index("core")
    models, slab, _ = grams.shape
    ny, nz, nx = (lax.axis_size(a) for a in ("y", "z", "x"))
    cols = weights.shape[2]
    half = models // 2
    turn = (x - y) % nx

    w_slots = all_shifts(weights, "y")

    chip_gram = core_pair(grams, 2)
    wide = chip_gram.shape[2]
    mine = lax.dynamic_slice_in_dim(chip_gram, core * half, half, 0)
    total = jnp.sum(chip_gram.astype(F32), axis=0).astype(BF16)
    mine, total = lax.optimization_barrier((mine, total))
    mine = lax.ppermute(
        mine, ("y", "x"), [(a * nx + b, b * nx + a) for a in range(ny) for b in range(nx)]
    )
    mine = jnp.stack(all_shifts(mine, "x"))
    gram_slots = core_pair(mine, 1)
    gram_slots = rolled(gram_slots, turn)

    total = lax.all_gather(total, "z", axis=0, tiled=True)
    rows = total.shape[0]
    total = lax.dynamic_slice_in_dim(total, core * (rows // 2), rows // 2, 0)
    total = jnp.stack(all_shifts(total, "x"))
    total = core_pair(total, 1)
    total = jnp.concatenate(rolled(total, turn), axis=1)

    product = jnp.einsum(
        "mkc,mkr->cr",
        jnp.concatenate(w_slots, axis=0),
        jnp.concatenate(gram_slots, axis=0),
        preferred_element_type=F32,
    )
    row_of = lax.broadcasted_iota(jnp.int32, (slab, wide), 0) + z * slab
    on_diag = row_of == lax.broadcasted_iota(jnp.int32, (slab, wide), 1)
    diag_part = jnp.where(on_diag[None], gram_slots[0], jnp.zeros((), BF16))
    diag_product = jnp.einsum(
        "mkc,mkr->cr", weights, diag_part, preferred_element_type=F32
    )
    part = 0.9 * product + 0.1 * diag_product
    right_side = lax.psum_scatter(part, "z", scatter_dimension=0, tiled=True)
    total_diag = jnp.sum(diag_part.astype(F32), axis=(0, 1))
    total_diag = lax.all_gather(total_diag, "z")
    total_diag = jnp.sum(total_diag, axis=0)[None]
    diag_rest = 0.9 * (total_diag - lax.reduce_precision(total_diag, 8, 7)) + 0.1 * total_diag

    def apply(direction):
        rounded = lax.optimization_barrier(direction.astype(BF16))
        everyone = jnp.concatenate(all_shifts(rounded, "y"), axis=1)
        product = lax.dot_general(
            everyone, total, (((1,), (1,)), ((), ())), preferred_element_type=F32
        )
        return 0.9 * product + diag_rest * rounded.astype(F32)

    def sums(*pairs):
        return jnp.stack([jnp.sum(a * b, axis=1) for a, b in pairs])

    mapped = apply(right_side)
    norm, curvature, square = y_sum(
        sums((right_side, right_side), (right_side, mapped), (mapped, mapped))
    )
    step = norm / curvature
    norm_next = norm - 2.0 * step * curvature + step * step * square
    merged = step[:, None] * right_side
    residual = right_side - step[:, None] * mapped
    direction = residual + (norm_next / norm)[:, None] * right_side
    mapped = apply(direction)
    norm, curvature = y_sum(sums((residual, residual), (direction, mapped)))
    step = norm / curvature
    merged = merged + step[:, None] * direction
    residual = residual - step[:, None] * mapped

    sent = jnp.stack([merged, residual]).reshape(2, cols // nz, nz, slab)
    sent = sent.transpose(2, 0, 3, 1)
    got = lax.all_to_all(sent, "z", 0, 0, tiled=True)
    got = got.transpose(1, 2, 0, 3).reshape(2, slab, cols)
    return got[0], got[1]


def solution(mesh):
    torus = Mesh(mesh.devices.reshape(4, 8, 4, 2), ("y", "z", "x", "core"))
    spec_in = P(None, ("y", "z"), ("x", "core"))
    spec_out = P(("y", "z"), ("x", "core"))
    return jax.shard_map(
        shards,
        mesh=torus,
        in_specs=(spec_in, spec_in),
        out_specs=(spec_out, spec_out),
        check_vma=False,
    )
```

```python
import jax
import jax.numpy as jnp
from jax import lax
from jax.experimental import pallas as pl
from jax.experimental.pallas import tpu as pltpu
from jax.sharding import Mesh
from jax.sharding import PartitionSpec as P


F32, BF16 = jnp.float32, jnp.bfloat16


def shift(x, axis, by):
    size = lax.axis_size(axis)
    return lax.ppermute(x, axis, [(i, (i + by) % size) for i in range(size)])


def all_shifts(x, axis):
    return [x] + [shift(x, axis, by) for by in range(1, lax.axis_size(axis))]


def core_pair(x, axis):
    other = shift(x, "core", 1)
    first = lax.axis_index("core") == 0
    return jnp.concatenate(
        [jnp.where(first, x, other), jnp.where(first, other, x)], axis=axis
    )


def rolled(blocks, start):
    n = blocks.shape[0]
    return [
        lax.dynamic_index_in_dim(blocks, (start + i) % n, 0, keepdims=False) for i in range(n)
    ]


def y_sum(parts):
    return sum(all_shifts(parts, "y"))


def ring_scatter(parts):
    z, n = lax.axis_index("z"), lax.axis_size("z")
    far = n // 2
    rows = parts.shape[1]
    mid = rows // 2

    def part(dest):
        return lax.dynamic_index_in_dim(parts, (z + dest) % n, 0, keepdims=False)

    opposite = part(far)
    down, up = shift(opposite[:mid], "z", -1), shift(opposite[mid:], "z", 1)
    for hops in range(far - 1, 0, -1):
        down, up = lax.optimization_barrier((down, up))
        if hops == far - 1:
            down = jnp.pad(down, ((0, rows - mid), (0, 0)))
            up = jnp.pad(up, ((mid, 0), (0, 0)))
        down = shift(part(-hops) + down, "z", -1)
        up = shift(part(hops) + up, "z", 1)
    return part(0) + down + up


def in_row_order(ours, theirs, deep):
    blocks, _, wide = ours.shape

    def kernel(ours_ref, theirs_ref, out_ref, sems):
        y, x, core = (lax.axis_index(a) for a in ("y", "x", "core"))
        copies = []
        for slot in range(blocks):
            to = lax.rem(slot + y - x + blocks, blocks) * 2
            for i, ref in enumerate((ours_ref, theirs_ref)):
                half = core if i == 0 else 1 - core
                copies.append(
                    pltpu.make_async_copy(
                        ref.at[slot, pl.ds(0, deep)],
                        out_ref.at[to + half],
                        sems.at[slot * 2 + i],
                    )
                )
        for copy in copies:
            copy.start()
        for copy in copies:
            copy.wait()

    out = pl.pallas_call(
        kernel,
        out_shape=jax.ShapeDtypeStruct((2 * blocks, deep, wide), ours.dtype),
        in_specs=[pl.BlockSpec(memory_space=pl.ANY)] * 2,
        out_specs=pl.BlockSpec(memory_space=pltpu.VMEM),
        scratch_shapes=[pltpu.SemaphoreType.DMA((2 * blocks,))],
        name="in_row_order",
    )(ours, theirs)
    return out.reshape(2 * blocks * deep, wide)


def shards(grams, weights):
    y, z, x = (lax.axis_index(a) for a in ("y", "z", "x"))
    core = lax.axis_index("core")
    models, slab, _ = grams.shape
    ny, nz, nx = (lax.axis_size(a) for a in ("y", "z", "x"))
    cols = weights.shape[2]
    half = models // 2
    turn = (x - y) % nx

    w_slots = all_shifts(weights, "y")

    chip_gram = core_pair(grams, 2)
    wide = chip_gram.shape[2]
    mine = lax.dynamic_slice_in_dim(chip_gram, core * half, half, 0)

    total = jnp.sum(grams.astype(F32), axis=0)
    row_of = lax.broadcasted_iota(jnp.int32, (slab, wide), 0) + z * slab
    on_diag = row_of == lax.broadcasted_iota(jnp.int32, (slab, wide), 1)
    col_of = lax.broadcasted_iota(jnp.int32, total.shape, 1) + core * (wide // 2)
    block_diag = (row_of[:, : wide // 2] == col_of) & (x == y)
    diag = jnp.sum(jnp.where(block_diag, total, 0.0), axis=0)
    high = lax.reduce_precision(diag, 8, 7)
    middle = lax.reduce_precision(diag - high, 8, 7)
    low = diag - high - middle
    tail = jnp.concatenate([jnp.stack([high, middle, low]), jnp.zeros((5, wide // 2), F32)])
    total = jnp.concatenate([total, tail], axis=0).astype(BF16)
    mine, total = lax.optimization_barrier((mine, total))

    mine = lax.ppermute(
        mine, ("y", "x"), [(a * nx + b, b * nx + a) for a in range(ny) for b in range(nx)]
    )
    total = lax.all_gather(total, "z")
    mine = jnp.stack(all_shifts(mine, "x"))
    gram_slots = core_pair(mine, 1)
    gram_slots = rolled(gram_slots, turn)

    tail = total[:, slab:].astype(F32).sum(axis=0)
    blank = jnp.zeros_like(tail)
    tail = jnp.concatenate(
        [jnp.where(core == 0, tail, blank), jnp.where(core == 0, blank, tail)], axis=1
    )
    total = total[:, :slab].reshape(nz * slab, -1).T
    deep = total.shape[0]
    total = jnp.concatenate([total, tail.astype(BF16)], axis=0)
    ours = jnp.stack(all_shifts(total, "x"))
    theirs = shift(ours, "core", 1)
    tail = sum(
        lax.dynamic_index_in_dim(t, turn, 0, keepdims=False)[deep:].astype(F32)
        for t in (ours, theirs)
    )
    total = in_row_order(ours, theirs, deep)
    total_diag = jnp.sum(tail, axis=0)[None]
    diag_rest = 0.9 * (total_diag - tail[:1]) + 0.1 * total_diag

    product = jnp.einsum(
        "mkc,mkr->cr",
        jnp.concatenate(w_slots, axis=0),
        jnp.concatenate(gram_slots, axis=0),
        preferred_element_type=F32,
    )
    diag_part = jnp.where(on_diag[None], gram_slots[0], jnp.zeros((), BF16))
    diag_product = jnp.einsum(
        "mkc,mkr->cr", weights, diag_part, preferred_element_type=F32
    )
    part = 0.9 * product + 0.1 * diag_product
    right_side = ring_scatter(part.reshape(nz, cols // nz, -1))

    def apply(direction):
        rounded = lax.optimization_barrier(direction.astype(BF16))
        everyone = jnp.concatenate(all_shifts(rounded, "y"), axis=1)
        product = jnp.dot(everyone, total, preferred_element_type=F32)
        return 0.9 * product + diag_rest * rounded.astype(F32)

    def sums(*pairs):
        return jnp.stack([jnp.sum(a * b, axis=1) for a, b in pairs])

    mapped = apply(right_side)
    norm, curvature, square = y_sum(
        sums((right_side, right_side), (right_side, mapped), (mapped, mapped))
    )
    step = norm / curvature
    norm_next = norm - 2.0 * step * curvature + step * step * square
    merged = step[:, None] * right_side
    residual = right_side - step[:, None] * mapped
    direction = residual + (norm_next / norm)[:, None] * right_side
    mapped = apply(direction)
    norm, curvature = y_sum(sums((residual, residual), (direction, mapped)))
    step = norm / curvature
    merged = merged + step[:, None] * direction
    residual = residual - step[:, None] * mapped

    sent = jnp.stack([merged, residual]).reshape(2, cols // nz, nz, slab)
    sent = sent.transpose(2, 0, 3, 1)
    got = lax.all_to_all(sent, "z", 0, 0, tiled=True)
    got = got.transpose(1, 2, 0, 3).reshape(2, slab, cols)
    return got[0], got[1]


def solution(mesh):
    torus = Mesh(mesh.devices.reshape(4, 8, 4, 2), ("y", "z", "x", "core"))
    spec_in = P(None, ("y", "z"), ("x", "core"))
    spec_out = P(("y", "z"), ("x", "core"))
    return jax.shard_map(
        shards,
        mesh=torus,
        in_specs=(spec_in, spec_in),
        out_specs=(spec_out, spec_out),
        check_vma=False,
    )
```

```python
import jax
import jax.numpy as jnp
from jax import lax
from jax.experimental import pallas as pl
from jax.experimental.pallas import tpu as pltpu
from jax.sharding import Mesh
from jax.sharding import PartitionSpec as P


F32, BF16 = jnp.float32, jnp.bfloat16


def shift(x, axis, by):
    size = lax.axis_size(axis)
    return lax.ppermute(x, axis, [(i, (i + by) % size) for i in range(size)])


def all_shifts(x, axis):
    return [x] + [shift(x, axis, by) for by in range(1, lax.axis_size(axis))]


def core_pair(x, axis):
    other = shift(x, "core", 1)
    first = lax.axis_index("core") == 0
    return jnp.concatenate(
        [jnp.where(first, x, other), jnp.where(first, other, x)], axis=axis
    )


def rolled(blocks, start):
    n = blocks.shape[0]
    return [
        lax.dynamic_index_in_dim(blocks, (start + i) % n, 0, keepdims=False) for i in range(n)
    ]


def y_sum(parts):
    return sum(all_shifts(parts, "y"))


def ring_scatter(parts):
    z, n = lax.axis_index("z"), lax.axis_size("z")
    far = n // 2
    rows = parts.shape[1]
    mid = rows // 2

    def part(dest):
        return lax.dynamic_index_in_dim(parts, (z + dest) % n, 0, keepdims=False)

    opposite = part(far)
    down, up = shift(opposite[:mid], "z", -1), shift(opposite[mid:], "z", 1)
    for hops in range(far - 1, 0, -1):
        down, up = lax.optimization_barrier((down, up))
        if hops == far - 1:
            down = jnp.pad(down, ((0, rows - mid), (0, 0)))
            up = jnp.pad(up, ((mid, 0), (0, 0)))
        down = shift(part(-hops) + down, "z", -1)
        up = shift(part(hops) + up, "z", 1)
    return part(0) + down + up


def in_row_order(ours, theirs, deep):
    blocks, _, wide = ours.shape

    def kernel(ours_ref, theirs_ref, out_ref, sems):
        y, x, core = (lax.axis_index(a) for a in ("y", "x", "core"))
        copies = []
        for slot in range(blocks):
            to = lax.rem(slot + y - x + blocks, blocks) * 2
            for i, ref in enumerate((ours_ref, theirs_ref)):
                half = core if i == 0 else 1 - core
                copies.append(
                    pltpu.make_async_copy(
                        ref.at[slot, pl.ds(0, deep)],
                        out_ref.at[to + half],
                        sems.at[slot * 2 + i],
                    )
                )
        for copy in copies:
            copy.start()
        for copy in copies:
            copy.wait()

    out = pl.pallas_call(
        kernel,
        out_shape=jax.ShapeDtypeStruct((2 * blocks, deep, wide), ours.dtype),
        in_specs=[pl.BlockSpec(memory_space=pl.ANY)] * 2,
        out_specs=pl.BlockSpec(memory_space=pltpu.VMEM),
        scratch_shapes=[pltpu.SemaphoreType.DMA((2 * blocks,))],
        name="in_row_order",
    )(ours, theirs)
    return out.reshape(2 * blocks * deep, wide)


def shards(grams, weights):
    y, z, x = (lax.axis_index(a) for a in ("y", "z", "x"))
    core = lax.axis_index("core")
    models, slab, _ = grams.shape
    ny, nz, nx = (lax.axis_size(a) for a in ("y", "z", "x"))
    cols = weights.shape[2]
    half = models // 2
    turn = (x - y) % nx

    w_slots = all_shifts(weights, "y")

    chip_gram = core_pair(grams, 2)
    wide = chip_gram.shape[2]
    mine = lax.dynamic_slice_in_dim(chip_gram, core * half, half, 0)

    total = jnp.sum(grams.astype(F32), axis=0)
    row_of = lax.broadcasted_iota(jnp.int32, (slab, wide), 0) + z * slab
    on_diag = row_of == lax.broadcasted_iota(jnp.int32, (slab, wide), 1)
    col_of = lax.broadcasted_iota(jnp.int32, total.shape, 1) + core * (wide // 2)
    block_diag = (row_of[:, : wide // 2] == col_of) & (x == y)
    diag = jnp.sum(jnp.where(block_diag, total, 0.0), axis=0)
    high = lax.reduce_precision(diag, 8, 7)
    middle = lax.reduce_precision(diag - high, 8, 7)
    low = diag - high - middle
    tail = jnp.concatenate([jnp.stack([high, middle, low]), jnp.zeros((5, wide // 2), F32)])
    total = jnp.concatenate([total, tail], axis=0).astype(BF16)
    mine, total = lax.optimization_barrier((mine, total))

    mine = lax.ppermute(
        mine, ("y", "x"), [(a * nx + b, b * nx + a) for a in range(ny) for b in range(nx)]
    )
    total = jnp.broadcast_to(total, (nz, *total.shape))
    total = lax.all_to_all(total, "z", 0, 0, tiled=True)
    mine = jnp.stack(all_shifts(mine, "x"))
    gram_slots = core_pair(mine, 1)
    gram_slots = rolled(gram_slots, turn)

    tail = total[:, slab:].astype(F32).sum(axis=0)
    blank = jnp.zeros_like(tail)
    tail = jnp.concatenate(
        [jnp.where(core == 0, tail, blank), jnp.where(core == 0, blank, tail)], axis=1
    )
    total = total[:, :slab].reshape(nz * slab, -1).T
    deep = total.shape[0]
    total = jnp.concatenate([total, tail.astype(BF16)], axis=0)
    ours = jnp.stack(all_shifts(total, "x"))
    theirs = shift(ours, "core", 1)
    tail = sum(
        lax.dynamic_index_in_dim(t, turn, 0, keepdims=False)[deep:].astype(F32)
        for t in (ours, theirs)
    )
    total = in_row_order(ours, theirs, deep)
    total_diag = jnp.sum(tail, axis=0)[None]
    diag_rest = 0.9 * (total_diag - tail[:1]) + 0.1 * total_diag

    product = jnp.einsum(
        "mkc,mkr->cr",
        jnp.concatenate(w_slots, axis=0),
        jnp.concatenate(gram_slots, axis=0),
        preferred_element_type=F32,
    )
    diag_part = jnp.where(on_diag[None], gram_slots[0], jnp.zeros((), BF16))
    diag_product = jnp.einsum(
        "mkc,mkr->cr", weights, diag_part, preferred_element_type=F32
    )
    part = 0.9 * product + 0.1 * diag_product
    right_side = ring_scatter(part.reshape(nz, cols // nz, -1))

    def apply(direction):
        rounded = lax.optimization_barrier(direction.astype(BF16))
        everyone = jnp.concatenate(all_shifts(rounded, "y"), axis=1)
        product = jnp.dot(everyone, total, preferred_element_type=F32)
        return 0.9 * product + diag_rest * rounded.astype(F32)

    def sums(*pairs):
        return jnp.stack([jnp.sum(a * b, axis=1) for a, b in pairs])

    mapped = apply(right_side)
    norm, curvature, square = y_sum(
        sums((right_side, right_side), (right_side, mapped), (mapped, mapped))
    )
    step = norm / curvature
    norm_next = norm - 2.0 * step * curvature + step * step * square
    merged = step[:, None] * right_side
    residual = right_side - step[:, None] * mapped
    direction = residual + (norm_next / norm)[:, None] * right_side
    mapped = apply(direction)
    norm, curvature = y_sum(sums((residual, residual), (direction, mapped)))
    step = norm / curvature
    merged = merged + step[:, None] * direction
    residual = residual - step[:, None] * mapped

    sent = jnp.stack([merged, residual]).astype(BF16).reshape(2, cols // nz, nz, slab)
    sent = sent.transpose(2, 0, 3, 1)
    got = lax.all_to_all(sent, "z", 0, 0, tiled=True)
    got = got.transpose(1, 2, 0, 3).reshape(2, slab, cols)
    return got[0].astype(F32), got[1].astype(F32)


def solution(mesh):
    torus = Mesh(mesh.devices.reshape(4, 8, 4, 2), ("y", "z", "x", "core"))
    spec_in = P(None, ("y", "z"), ("x", "core"))
    spec_out = P(("y", "z"), ("x", "core"))
    return jax.shard_map(
        shards,
        mesh=torus,
        in_specs=(spec_in, spec_in),
        out_specs=(spec_out, spec_out),
        check_vma=False,
    )
```

```python
import jax
import jax.numpy as jnp
from jax import lax
from jax.experimental import pallas as pl
from jax.experimental.pallas import tpu as pltpu
from jax.sharding import Mesh
from jax.sharding import PartitionSpec as P


F32, BF16 = jnp.float32, jnp.bfloat16


def shift(x, axis, by):
    size = lax.axis_size(axis)
    return lax.ppermute(x, axis, [(i, (i + by) % size) for i in range(size)])


def all_shifts(x, axis):
    return [x] + [shift(x, axis, by) for by in range(1, lax.axis_size(axis))]


def core_pair(x, axis):
    other = shift(x, "core", 1)
    first = lax.axis_index("core") == 0
    return jnp.concatenate(
        [jnp.where(first, x, other), jnp.where(first, other, x)], axis=axis
    )


def rolled(blocks, start):
    n = blocks.shape[0]
    return [
        lax.dynamic_index_in_dim(blocks, (start + i) % n, 0, keepdims=False) for i in range(n)
    ]


def y_sum(parts):
    return sum(all_shifts(parts, "y"))


def ring_scatter(parts):
    z, n = lax.axis_index("z"), lax.axis_size("z")
    far = n // 2
    rows = parts.shape[1]
    mid = rows // 2

    def part(dest):
        return lax.dynamic_index_in_dim(parts, (z + dest) % n, 0, keepdims=False)

    opposite = part(far)
    down, up = shift(opposite[:mid], "z", -1), shift(opposite[mid:], "z", 1)
    for hops in range(far - 1, 0, -1):
        down, up = lax.optimization_barrier((down, up))
        if hops == far - 1:
            down = jnp.pad(down, ((0, rows - mid), (0, 0)))
            up = jnp.pad(up, ((mid, 0), (0, 0)))
        down = shift(part(-hops) + down, "z", -1)
        up = shift(part(hops) + up, "z", 1)
    return part(0) + down + up


def in_row_order(ours, theirs, deep):
    blocks, _, wide = ours.shape

    def kernel(ours_ref, theirs_ref, out_ref, sems):
        y, x, core = (lax.axis_index(a) for a in ("y", "x", "core"))
        copies = []
        for slot in range(blocks):
            to = lax.rem(slot + y - x + blocks, blocks) * 2
            for i, ref in enumerate((ours_ref, theirs_ref)):
                half = core if i == 0 else 1 - core
                copies.append(
                    pltpu.make_async_copy(
                        ref.at[slot, pl.ds(0, deep)],
                        out_ref.at[to + half],
                        sems.at[slot * 2 + i],
                    )
                )
        for copy in copies:
            copy.start()
        for copy in copies:
            copy.wait()

    out = pl.pallas_call(
        kernel,
        out_shape=jax.ShapeDtypeStruct((2 * blocks, deep, wide), ours.dtype),
        in_specs=[pl.BlockSpec(memory_space=pl.ANY)] * 2,
        out_specs=pl.BlockSpec(memory_space=pltpu.VMEM),
        scratch_shapes=[pltpu.SemaphoreType.DMA((2 * blocks,))],
        name="in_row_order",
    )(ours, theirs)
    return out.reshape(2 * blocks * deep, wide)


def shards(grams, weights):
    y, z, x = (lax.axis_index(a) for a in ("y", "z", "x"))
    core = lax.axis_index("core")
    slab, wide = grams.shape[1], 2 * grams.shape[2]
    ny, nz, nx = (lax.axis_size(a) for a in ("y", "z", "x"))
    cols = weights.shape[2]
    turn = (x - y) % nx

    w_slots = all_shifts(weights, "y")

    total = jnp.sum(grams.astype(F32), axis=0)
    row_of = lax.broadcasted_iota(jnp.int32, (slab, wide), 0) + z * slab
    on_diag = row_of == lax.broadcasted_iota(jnp.int32, (slab, wide), 1)
    col_of = lax.broadcasted_iota(jnp.int32, total.shape, 1) + core * (wide // 2)
    block_diag = (row_of[:, : wide // 2] == col_of) & (x == y)
    diag = jnp.sum(jnp.where(block_diag, total, 0.0), axis=0)
    high = lax.reduce_precision(diag, 8, 7)
    middle = lax.reduce_precision(diag - high, 8, 7)
    low = diag - high - middle
    tail = jnp.concatenate([jnp.stack([high, middle, low]), jnp.zeros((5, wide // 2), F32)])
    total = jnp.concatenate([total, tail], axis=0).astype(BF16)

    mine = lax.ppermute(
        grams, ("y", "x"), [(a * nx + b, b * nx + a) for a in range(ny) for b in range(nx)]
    )
    total = jnp.broadcast_to(total, (nz, *total.shape))
    total = lax.all_to_all(total, "z", 0, 0, tiled=True)
    mine = jnp.stack(all_shifts(mine, "x"))
    gram_slots = core_pair(mine, 3)
    gram_slots = rolled(gram_slots, turn)

    tail = total[:, slab:].astype(F32).sum(axis=0)
    blank = jnp.zeros_like(tail)
    tail = jnp.concatenate(
        [jnp.where(core == 0, tail, blank), jnp.where(core == 0, blank, tail)], axis=1
    )
    total = total[:, :slab].reshape(nz * slab, -1).T
    deep = total.shape[0]
    total = jnp.concatenate([total, tail.astype(BF16)], axis=0)
    ours = jnp.stack(all_shifts(total, "x"))
    theirs = shift(ours, "core", 1)
    tail = sum(
        lax.dynamic_index_in_dim(t, turn, 0, keepdims=False)[deep:].astype(F32)
        for t in (ours, theirs)
    )
    total = in_row_order(ours, theirs, deep)
    total_diag = jnp.sum(tail, axis=0)[None]
    diag_rest = 0.9 * (total_diag - tail[:1]) + 0.1 * total_diag

    product = jnp.einsum(
        "mkc,mkr->cr",
        jnp.concatenate(w_slots, axis=0),
        jnp.concatenate(gram_slots, axis=0),
        preferred_element_type=F32,
    )
    diag_part = jnp.where(on_diag[None], gram_slots[0], jnp.zeros((), BF16))
    diag_product = jnp.einsum(
        "mkc,mkr->cr", weights, diag_part, preferred_element_type=F32
    )
    part = 0.9 * product + 0.1 * diag_product
    right_side = ring_scatter(part.reshape(nz, cols // nz, -1))

    def apply(direction):
        rounded = lax.optimization_barrier(direction.astype(BF16))
        everyone = jnp.concatenate(all_shifts(rounded, "y"), axis=1)
        product = jnp.dot(everyone, total, preferred_element_type=F32)
        return 0.9 * product + diag_rest * rounded.astype(F32)

    def sums(*pairs):
        return jnp.stack([jnp.sum(a * b, axis=1) for a, b in pairs])

    mapped = apply(right_side)
    norm, curvature, square = y_sum(
        sums((right_side, right_side), (right_side, mapped), (mapped, mapped))
    )
    step = norm / curvature
    norm_next = norm - 2.0 * step * curvature + step * step * square
    merged = step[:, None] * right_side
    residual = right_side - step[:, None] * mapped
    direction = residual + (norm_next / norm)[:, None] * right_side
    mapped = apply(direction)
    norm, curvature = y_sum(sums((residual, residual), (direction, mapped)))
    step = norm / curvature
    merged = merged + step[:, None] * direction
    residual = residual - step[:, None] * mapped

    sent = jnp.stack([merged, residual]).astype(BF16).reshape(2, cols // nz, nz, slab)
    sent = sent.transpose(2, 0, 3, 1)
    got = lax.all_to_all(sent, "z", 0, 0, tiled=True)
    got = got.transpose(1, 2, 0, 3).reshape(2, slab, cols)
    return got[0].astype(F32), got[1].astype(F32)


def solution(mesh):
    torus = Mesh(mesh.devices.reshape(4, 8, 4, 2), ("y", "z", "x", "core"))
    spec_in = P(None, ("y", "z"), ("x", "core"))
    spec_out = P(("y", "z"), ("x", "core"))
    return jax.shard_map(
        shards,
        mesh=torus,
        in_specs=(spec_in, spec_in),
        out_specs=(spec_out, spec_out),
        check_vma=False,
    )
```

```python
import jax
import jax.numpy as jnp
from jax import lax
from jax.experimental import pallas as pl
from jax.experimental.pallas import tpu as pltpu
from jax.sharding import Mesh
from jax.sharding import PartitionSpec as P


F32, BF16 = jnp.float32, jnp.bfloat16


def shift(x, axis, by):
    size = lax.axis_size(axis)
    return lax.ppermute(x, axis, [(i, (i + by) % size) for i in range(size)])


def all_shifts(x, axis):
    return [x] + [shift(x, axis, by) for by in range(1, lax.axis_size(axis))]


def core_pair(x, axis):
    other = shift(x, "core", 1)
    first = lax.axis_index("core") == 0
    return jnp.concatenate(
        [jnp.where(first, x, other), jnp.where(first, other, x)], axis=axis
    )


def rolled(blocks, start):
    n = blocks.shape[0]
    return [
        lax.dynamic_index_in_dim(blocks, (start + i) % n, 0, keepdims=False) for i in range(n)
    ]


def y_sum(parts):
    return sum(all_shifts(parts, "y"))


def ring_scatter(parts):
    z, n = lax.axis_index("z"), lax.axis_size("z")
    far = n // 2
    rows = parts.shape[1]
    mid = rows // 2

    def part(dest):
        return lax.dynamic_index_in_dim(parts, (z + dest) % n, 0, keepdims=False)

    opposite = part(far)
    down, up = shift(opposite[:mid], "z", -1), shift(opposite[mid:], "z", 1)
    for hops in range(far - 1, 0, -1):
        down, up = lax.optimization_barrier((down, up))
        if hops == far - 1:
            down = jnp.pad(down, ((0, rows - mid), (0, 0)))
            up = jnp.pad(up, ((mid, 0), (0, 0)))
        down = shift(part(-hops) + down, "z", -1)
        up = shift(part(hops) + up, "z", 1)
    return part(0) + down + up


def in_row_order(ours, theirs, deep):
    blocks, _, wide = ours.shape

    def kernel(ours_ref, theirs_ref, out_ref, sems):
        y, x, core = (lax.axis_index(a) for a in ("y", "x", "core"))
        copies = []
        for slot in range(blocks):
            to = lax.rem(slot + y - x + blocks, blocks) * 2
            for i, ref in enumerate((ours_ref, theirs_ref)):
                half = core if i == 0 else 1 - core
                copies.append(
                    pltpu.make_async_copy(
                        ref.at[slot, pl.ds(0, deep)],
                        out_ref.at[to + half],
                        sems.at[slot * 2 + i],
                    )
                )
        for copy in copies:
            copy.start()
        for copy in copies:
            copy.wait()

    out = pl.pallas_call(
        kernel,
        out_shape=jax.ShapeDtypeStruct((2 * blocks, deep, wide), ours.dtype),
        in_specs=[pl.BlockSpec(memory_space=pl.ANY)] * 2,
        out_specs=pl.BlockSpec(memory_space=pltpu.VMEM),
        scratch_shapes=[pltpu.SemaphoreType.DMA((2 * blocks,))],
        name="in_row_order",
    )(ours, theirs)
    return out.reshape(2 * blocks * deep, wide)


def shards(grams, weights):
    y, z, x = (lax.axis_index(a) for a in ("y", "z", "x"))
    core = lax.axis_index("core")
    slab, wide = grams.shape[1], 2 * grams.shape[2]
    ny, nz, nx = (lax.axis_size(a) for a in ("y", "z", "x"))
    cols = weights.shape[2]
    turn = (x - y) % nx

    w_slots = all_shifts(weights, "y")

    total = jnp.sum(grams.astype(F32), axis=0)
    row_of = lax.broadcasted_iota(jnp.int32, (slab, wide), 0) + z * slab
    on_diag = row_of == lax.broadcasted_iota(jnp.int32, (slab, wide), 1)
    col_of = lax.broadcasted_iota(jnp.int32, total.shape, 1) + core * (wide // 2)
    block_diag = (row_of[:, : wide // 2] == col_of) & (x == y)
    diag = jnp.sum(jnp.where(block_diag, total, 0.0), axis=0)
    high = lax.reduce_precision(diag, 8, 7)
    middle = lax.reduce_precision(diag - high, 8, 7)
    low = diag - high - middle
    tail = jnp.concatenate([jnp.stack([high, middle, low]), jnp.zeros((5, wide // 2), F32)])
    total = jnp.concatenate([total, tail], axis=0).astype(BF16)

    mine = lax.ppermute(
        grams, ("y", "x"), [(a * nx + b, b * nx + a) for a in range(ny) for b in range(nx)]
    )
    total = jnp.broadcast_to(total, (nz, *total.shape))
    total = lax.all_to_all(total, "z", 0, 0, tiled=True)
    mine = jnp.stack(all_shifts(mine, "x"))
    gram_slots = core_pair(mine, 3)
    gram_slots = rolled(gram_slots, turn)

    tail = total[:, slab:].astype(F32).sum(axis=0)
    blank = jnp.zeros_like(tail)
    tail = jnp.concatenate(
        [jnp.where(core == 0, tail, blank), jnp.where(core == 0, blank, tail)], axis=1
    )
    total = total[:, :slab].reshape(nz * slab, -1).T
    deep = total.shape[0]
    total = jnp.concatenate([total, tail.astype(BF16)], axis=0)
    ours = jnp.stack(all_shifts(total, "x"))
    theirs = shift(ours, "core", 1)
    tail = sum(
        lax.dynamic_index_in_dim(t, turn, 0, keepdims=False)[deep:].astype(F32)
        for t in (ours, theirs)
    )
    total = in_row_order(ours, theirs, deep)
    total_diag = jnp.sum(tail, axis=0)[None]
    this = lax.broadcasted_iota(jnp.int32, total.shape, 0)
    that = lax.broadcasted_iota(jnp.int32, total.shape, 1)
    total = jnp.where(this == that, jnp.zeros((), BF16), total)
    total = lax.optimization_barrier(total)

    product = jnp.einsum(
        "mkc,mkr->cr",
        jnp.concatenate(w_slots, axis=0),
        jnp.concatenate(gram_slots, axis=0),
        preferred_element_type=F32,
    )
    diag_part = jnp.where(on_diag[None], gram_slots[0], jnp.zeros((), BF16))
    diag_product = jnp.einsum(
        "mkc,mkr->cr", weights, diag_part, preferred_element_type=F32
    )
    part = 0.9 * product + 0.1 * diag_product
    right_side = ring_scatter(part.reshape(nz, cols // nz, -1))

    def apply(direction):
        rounded = lax.optimization_barrier(direction.astype(BF16))
        everyone = jnp.concatenate(all_shifts(rounded, "y"), axis=1)
        product = jnp.dot(everyone, total, preferred_element_type=F32)
        return 0.9 * product + total_diag * rounded.astype(F32)

    def sums(*pairs):
        return jnp.stack([jnp.sum(a * b, axis=1) for a, b in pairs])

    mapped = apply(right_side)
    norm, curvature, square = y_sum(
        sums((right_side, right_side), (right_side, mapped), (mapped, mapped))
    )
    step = norm / curvature
    norm_next = norm - 2.0 * step * curvature + step * step * square
    merged = step[:, None] * right_side
    residual = right_side - step[:, None] * mapped
    direction = residual + (norm_next / norm)[:, None] * right_side
    mapped = apply(direction)
    norm, curvature = y_sum(sums((residual, residual), (direction, mapped)))
    step = norm / curvature
    merged = merged + step[:, None] * direction
    residual = residual - step[:, None] * mapped

    sent = jnp.stack([merged, residual]).astype(BF16).reshape(2, cols // nz, nz, slab)
    sent = sent.transpose(2, 0, 3, 1)
    got = lax.all_to_all(sent, "z", 0, 0, tiled=True)
    got = got.transpose(1, 2, 0, 3).reshape(2, slab, cols)
    return got[0].astype(F32), got[1].astype(F32)


def solution(mesh):
    torus = Mesh(mesh.devices.reshape(4, 8, 4, 2), ("y", "z", "x", "core"))
    spec_in = P(None, ("y", "z"), ("x", "core"))
    spec_out = P(("y", "z"), ("x", "core"))
    return jax.shard_map(
        shards,
        mesh=torus,
        in_specs=(spec_in, spec_in),
        out_specs=(spec_out, spec_out),
        check_vma=False,
    )
```

```python
import jax
import jax.numpy as jnp
from jax import lax
from jax.experimental import pallas as pl
from jax.experimental.pallas import tpu as pltpu
from jax.sharding import Mesh
from jax.sharding import PartitionSpec as P


F32, BF16 = jnp.float32, jnp.bfloat16


def shift(x, axis, by):
    size = lax.axis_size(axis)
    return lax.ppermute(x, axis, [(i, (i + by) % size) for i in range(size)])


def all_shifts(x, axis):
    return [x] + [shift(x, axis, by) for by in range(1, lax.axis_size(axis))]


def core_pair(x, axis):
    other = shift(x, "core", 1)
    first = lax.axis_index("core") == 0
    return jnp.concatenate(
        [jnp.where(first, x, other), jnp.where(first, other, x)], axis=axis
    )


def rolled(blocks, start):
    n = blocks.shape[0]
    return [
        lax.dynamic_index_in_dim(blocks, (start + i) % n, 0, keepdims=False) for i in range(n)
    ]


def y_sum(parts):
    return sum(all_shifts(parts, "y"))


def ring_scatter(parts):
    z, n = lax.axis_index("z"), lax.axis_size("z")
    far = n // 2
    rows = parts.shape[1]
    mid = rows // 2

    def part(dest):
        return lax.dynamic_index_in_dim(parts, (z + dest) % n, 0, keepdims=False)

    opposite = part(far)
    down, up = shift(opposite[:mid], "z", -1), shift(opposite[mid:], "z", 1)
    for hops in range(far - 1, 0, -1):
        down, up = lax.optimization_barrier((down, up))
        if hops == far - 1:
            down = jnp.pad(down, ((0, rows - mid), (0, 0)))
            up = jnp.pad(up, ((mid, 0), (0, 0)))
        down = shift(part(-hops) + down, "z", -1)
        up = shift(part(hops) + up, "z", 1)
    return part(0) + down + up


def in_row_order(ours, theirs, deep):
    blocks, _, wide = ours.shape

    def kernel(ours_ref, theirs_ref, out_ref, sems):
        y, core = (lax.axis_index(a) for a in ("y", "core"))
        copies = []
        for slot in range(blocks):
            to = lax.rem(y - slot + blocks, blocks) * 2
            for i, ref in enumerate((ours_ref, theirs_ref)):
                half = core if i == 0 else 1 - core
                copies.append(
                    pltpu.make_async_copy(
                        ref.at[slot, pl.ds(0, deep)],
                        out_ref.at[to + half],
                        sems.at[slot * 2 + i],
                    )
                )
        for copy in copies:
            copy.start()
        for copy in copies:
            copy.wait()

    out = pl.pallas_call(
        kernel,
        out_shape=jax.ShapeDtypeStruct((2 * blocks, deep, wide), ours.dtype),
        in_specs=[pl.BlockSpec(memory_space=pl.ANY)] * 2,
        out_specs=pl.BlockSpec(memory_space=pltpu.VMEM),
        scratch_shapes=[pltpu.SemaphoreType.DMA((2 * blocks,))],
        name="in_row_order",
    )(ours, theirs)
    return out.reshape(2 * blocks * deep, wide)


def shards(grams, weights):
    y, z, x = (lax.axis_index(a) for a in ("y", "z", "x"))
    core = lax.axis_index("core")
    slab, wide = grams.shape[1], 2 * grams.shape[2]
    ny, nz, nx = (lax.axis_size(a) for a in ("y", "z", "x"))
    cols = weights.shape[2]
    turn = (x - y) % nx

    w_slots = all_shifts(weights, "y")

    total = jnp.sum(grams.astype(F32), axis=0)
    row_of = lax.broadcasted_iota(jnp.int32, (slab, wide), 0) + z * slab
    on_diag = row_of == lax.broadcasted_iota(jnp.int32, (slab, wide), 1)
    col_of = lax.broadcasted_iota(jnp.int32, total.shape, 1) + core * (wide // 2)
    block_diag = (row_of[:, : wide // 2] == col_of) & (x == y)
    diag = jnp.sum(jnp.where(block_diag, total, 0.0), axis=0)
    high = lax.reduce_precision(diag, 8, 7)
    middle = lax.reduce_precision(diag - high, 8, 7)
    low = diag - high - middle
    tail = jnp.concatenate([jnp.stack([high, middle, low]), jnp.zeros((5, wide // 2), F32)])
    total = jnp.concatenate([total, tail], axis=0).astype(BF16)

    mine = lax.ppermute(
        grams, ("y", "x"), [(a * nx + b, b * nx + a) for a in range(ny) for b in range(nx)]
    )
    total = jnp.broadcast_to(total, (nz, *total.shape))
    total = lax.all_to_all(total, "z", 0, 0, tiled=True)
    mine = jnp.stack(all_shifts(mine, "x"))
    gram_slots = core_pair(mine, 3)
    gram_slots = rolled(gram_slots, turn)

    tail = total[:, slab:].astype(F32).sum(axis=0)
    blank = jnp.zeros_like(tail)
    tail = jnp.concatenate(
        [jnp.where(core == 0, tail, blank), jnp.where(core == 0, blank, tail)], axis=1
    )
    total = total[:, :slab].reshape(nz * slab, -1).T
    deep = total.shape[0]
    total = jnp.concatenate([total, tail.astype(BF16)], axis=0)
    ours = jnp.broadcast_to(total, (nx, *total.shape))
    ours = lax.all_to_all(ours, "x", 0, 0, tiled=True)
    theirs = shift(ours, "core", 1)
    tail = sum(
        lax.dynamic_index_in_dim(t, y, 0, keepdims=False)[deep:].astype(F32)
        for t in (ours, theirs)
    )
    total = in_row_order(ours, theirs, deep)
    total_diag = jnp.sum(tail, axis=0)[None]
    this = lax.broadcasted_iota(jnp.int32, total.shape, 0)
    that = lax.broadcasted_iota(jnp.int32, total.shape, 1)
    total = jnp.where(this == that, jnp.zeros((), BF16), total)
    total = lax.optimization_barrier(total)

    product = jnp.einsum(
        "mkc,mkr->cr",
        jnp.concatenate(w_slots, axis=0),
        jnp.concatenate(gram_slots, axis=0),
        preferred_element_type=F32,
    )
    diag_part = jnp.where(on_diag[None], gram_slots[0], jnp.zeros((), BF16))
    diag_product = jnp.einsum(
        "mkc,mkr->cr", weights, diag_part, preferred_element_type=F32
    )
    part = 0.9 * product + 0.1 * diag_product
    right_side = ring_scatter(part.reshape(nz, cols // nz, -1))

    def apply(direction):
        rounded = lax.optimization_barrier(direction.astype(BF16))
        everyone = jnp.concatenate(all_shifts(rounded, "y"), axis=1)
        product = jnp.dot(everyone, total, preferred_element_type=F32)
        return 0.9 * product + total_diag * rounded.astype(F32)

    def sums(*pairs):
        return jnp.stack([jnp.sum(a * b, axis=1) for a, b in pairs])

    mapped = apply(right_side)
    norm, curvature, square = y_sum(
        sums((right_side, right_side), (right_side, mapped), (mapped, mapped))
    )
    step = norm / curvature
    norm_next = norm - 2.0 * step * curvature + step * step * square
    merged = step[:, None] * right_side
    residual = right_side - step[:, None] * mapped
    direction = residual + (norm_next / norm)[:, None] * right_side
    mapped = apply(direction)
    norm, curvature = y_sum(sums((residual, residual), (direction, mapped)))
    step = norm / curvature
    merged = merged + step[:, None] * direction
    residual = residual - step[:, None] * mapped

    sent = jnp.stack([merged, residual]).astype(BF16).reshape(2, cols // nz, nz, slab)
    sent = sent.transpose(2, 0, 3, 1)
    got = lax.all_to_all(sent, "z", 0, 0, tiled=True)
    got = got.transpose(1, 2, 0, 3).reshape(2, slab, cols)
    return got[0].astype(F32), got[1].astype(F32)


def solution(mesh):
    torus = Mesh(mesh.devices.reshape(4, 8, 4, 2), ("y", "z", "x", "core"))
    spec_in = P(None, ("y", "z"), ("x", "core"))
    spec_out = P(("y", "z"), ("x", "core"))
    return jax.shard_map(
        shards,
        mesh=torus,
        in_specs=(spec_in, spec_in),
        out_specs=(spec_out, spec_out),
        check_vma=False,
    )
```
